32 devices in a mesh: au: 4 (over y, x), vert: 8 (over z, core).
Axes of the slice: x: 2, y: 2, z: 4, core: 2. Of those that a mesh axis runs over, the one named last changes fastest.
Arguments:
- visibility: bfloat16 [2, 65536], P(None, ('au', 'vert')), may hold values from -6 to 6
- taps_u: bfloat16 [16, 65536], P(None, ('au', 'vert')), may hold values from 0.019897461 to 0.44921875
- taps_v: bfloat16 [16, 65536], P(None, ('au', 'vert')), may hold values from 0.019897461 to 0.44921875
- facet: int32 [65536, 1], P(('au', 'vert')), may hold values from 0 to 31; in each aligned block of 2048 rows (0 to 2047, 2048 to 4095, ...) at most 256 rows name the same one
- u_offset: int32 [65536], P(('au', 'vert')), may hold values from 0 to 2032
- v_offset: int32 [65536], P(('au', 'vert')), may hold values from 0 to 1008
Outputs:
- image: float32 [2, 8192, 8192], P(None, ('au', 'vert'))
The draws below stay inside these ranges and needn't reach their ends.
Inputs may be any that keep to these rules, and one draw needn't show every extreme that they name: Of the 2048 visibilities of one device at most 256 name the same facet, and some facet gets exactly 256 of some device's visibilities.
All inputs are finite; a program needn't handle non-finite values.
Results may differ from the reference program's by a relative error of at most 0.0058.
Values may be sent and summed in bfloat16 or wider, within the bound.
A program may use at most 128 MiB of HBM per device.

```python
import math
import jax
import jax.numpy as jnp
import numpy as np
from jax import lax

GRID = 8192
TAPS = 16
VIS_DEV = 2048
FACETS = 32
TU = 2048
TV = 1024
CAP = 256
VISIBILITIES = 65536
N_VERT = 8
DEVICES = 32


def touch_ends(result, own_key, smallest, high):
    spot = [jax.random.randint(jax.random.fold_in(own_key, axis), (), 0, length) for axis, length in enumerate(result.shape)]
    widest = result.shape.index(max(result.shape))
    neighbour = spot[:widest] + [(spot[widest] + 1) % result.shape[widest]] + spot[widest + 1:]
    return result.at[tuple(spot)].set(smallest).at[tuple(neighbour)].set(high)


def block_scale(stream_key, dims, split, least, largest):
    def one(position, shards_of):
        heights = jax.random.uniform(jax.random.fold_in(jax.random.fold_in(stream_key, 6), position), (shards_of,), jnp.float32, least / len(split), largest / len(split))
        return jnp.repeat(jnp.exp(heights), dims[position] // shards_of).reshape((-1,) + (1,) * (len(dims) - position - 1))

    level = one(*split[0])
    for cut in split[1:]:
        level = level * one(*cut)
    return level


def deal_out(stream_key, own, number, rows, count, top, bound, lean):
    sequence = jax.random.permutation(stream_key, count)
    crowded, ordinary = shares(count, rows * top, bound, lean, True), shares(count, rows * top, bound, lean, False)
    places = jnp.arange(count)

    def named(tallies, offset_by):
        used = int((tallies > 0).sum())
        fixed = max(1, used // 4)
        moved = fixed + (places - fixed + offset_by * (used - fixed)) % max(1, count - fixed)
        return jnp.zeros((count,), jnp.int32).at[sequence[jnp.where(places < fixed, places, moved)]].set(jnp.asarray(tallies, jnp.int32))

    tallies = jnp.where(number % 4 == 0, named(crowded, number // 4), named(ordinary, number - number // 4 - 1))
    mixed = jax.random.permutation(jax.random.fold_in(own, 3), count)
    donor, receiver = mixed[0:count // 2 * 2:2], mixed[1:count // 2 * 2:2]
    slack = jnp.minimum(tallies[donor] - 1, bound - tallies[receiver]) // 2
    slack = jnp.where((donor == sequence[0]) | (receiver == sequence[0]) | (tallies[receiver] == 0), 0, jnp.maximum(slack, 0))
    moved = jax.random.randint(jax.random.fold_in(own, 4), (count // 2,), 0, 1 << 20) % (slack + 1)
    tallies = tallies.at[donor].add(-moved).at[receiver].add(moved)
    items = jnp.searchsorted(jnp.cumsum(tallies), jnp.arange(rows * top), side="right").astype(jnp.int32)
    table = items.reshape(top, rows).T
    table = table[jax.random.permutation(jax.random.fold_in(own, 1), rows)]
    offset_by = jax.random.randint(jax.random.fold_in(own, 2), (rows, 1), 0, top)
    return jnp.take_along_axis(table, (jnp.arange(top)[None, :] + offset_by) % top, axis=1)


def shares(amount, total, bound, slope, full):
    loads = [(1 << 20) // math.isqrt(standing ** slope) + 1 for standing in range(1, amount + 1)]
    largest = bound if full else min(bound, max(-(-total // amount), total * loads[0] // sum(loads)))
    least = 1 if total - largest >= amount - 1 else 0
    given, spare = [largest] + [least] * (amount - 1), total - largest - least * (amount - 1)
    while spare > 0:
        candidates = [i for i in range(1, amount) if given[i] < largest] or [i for i in range(1, amount) if given[i] < bound]
        mass, left = sum([loads[i] for i in candidates]), spare
        for i in candidates:
            extra = min(bound - given[i], max(1, left * loads[i] // mass), spare)
            given[i] = given[i] + extra
            spare = spare - extra
    return np.array(given)


def bell_draw(key, shape, spread, limit, pieces=(), kind=jnp.bfloat16):
    result = spread * jax.random.normal(key, shape, jnp.float32)
    if pieces:
        result = result * block_scale(key, shape, pieces, -0.22, 0.18)
    return jnp.clip(result, -limit, limit).astype(kind)


def setup_inputs(seed: int = 0) -> dict:
    arg_keys = jax.random.split(jax.random.key(seed), 7)
    visibility = bell_draw(arg_keys[0], (2, VISIBILITIES), 1.0, 6.0, ((1, 32),))
    taps_u = jnp.clip(0.019897461 + 0.4293213 * jax.random.uniform(arg_keys[1], (TAPS, VISIBILITIES), jnp.float32) ** block_scale(arg_keys[1], (TAPS, VISIBILITIES), ((1, 32),), -0.2, 0.2), 0.019897461, 0.44921875).astype(jnp.bfloat16)
    taps_v = jnp.clip(0.019897461 + 0.4293213 * jax.random.uniform(arg_keys[2], (TAPS, VISIBILITIES), jnp.float32) ** block_scale(arg_keys[2], (TAPS, VISIBILITIES), ((1, 32),), -0.2, 0.2), 0.019897461, 0.44921875).astype(jnp.bfloat16)
    facet_keys = jax.random.split(jax.random.fold_in(arg_keys[3], 1), VISIBILITIES // VIS_DEV)
    facet_turns = jax.random.permutation(jax.random.fold_in(arg_keys[3], 3), VISIBILITIES // VIS_DEV)
    facet = jax.vmap(lambda own, number: deal_out(jax.random.fold_in(arg_keys[3], 2), own, number, VIS_DEV, FACETS, 1, CAP, 2))(facet_keys, facet_turns).reshape((VISIBILITIES, 1))
    u_offset = touch_ends(jax.random.randint(arg_keys[4], (VISIBILITIES,), 0, TU - TAPS + 1), jax.random.fold_in(arg_keys[4], 1), 0, TU - TAPS).astype(jnp.int32)
    v_offset = touch_ends(jax.random.randint(arg_keys[5], (VISIBILITIES,), 0, TV - TAPS + 1), jax.random.fold_in(arg_keys[5], 1), 0, TV - TAPS).astype(jnp.int32)
    return dict(visibility=visibility, taps_u=taps_u, taps_v=taps_v, facet=facet, u_offset=u_offset, v_offset=v_offset)


def reference(visibility, taps_u, taps_v, facet, u_offset, v_offset):
    tap = jnp.arange(TAPS, dtype=jnp.int32)
    vis_blocks = jnp.transpose(visibility.reshape(2, DEVICES, VIS_DEV), (1, 0, 2))
    tu_blocks = jnp.transpose(taps_u.reshape(TAPS, DEVICES, VIS_DEV), (1, 0, 2))
    tv_blocks = jnp.transpose(taps_v.reshape(TAPS, DEVICES, VIS_DEV), (1, 0, 2))
    facet_blocks = facet[:, 0].reshape(DEVICES, VIS_DEV)
    u_blocks = u_offset.reshape(DEVICES, VIS_DEV)
    v_blocks = v_offset.reshape(DEVICES, VIS_DEV)

    def accumulate(acc, items):
        vis, tu, tv, target, uo, vo = items
        kv = tv.astype(jnp.float32)
        weighted_re = lax.optimization_barrier((vis[0].astype(jnp.float32)[None, :] * kv).astype(jnp.bfloat16))
        weighted_im = lax.optimization_barrier((vis[1].astype(jnp.float32)[None, :] * kv).astype(jnp.bfloat16))
        ku = tu.astype(jnp.float32)
        rows = target // N_VERT * TU + uo
        cols = target % N_VERT * TV + vo
        row_cells = rows[None, :] + tap[:, None]
        col_cells = cols[None, :] + tap[:, None]
        value_re = ku[:, None, :] * weighted_re.astype(jnp.float32)[None, :, :]
        value_im = ku[:, None, :] * weighted_im.astype(jnp.float32)[None, :, :]
        row_index = jnp.broadcast_to(row_cells[:, None, :], value_re.shape)
        col_index = jnp.broadcast_to(col_cells[None, :, :], value_re.shape)
        acc = acc.at[0, row_index, col_index].add(value_re)
        acc = acc.at[1, row_index, col_index].add(value_im)
        return (acc, None)
    start = jnp.zeros((2, GRID, GRID), jnp.float32)
    grid, _ = lax.scan(accumulate, start, (vis_blocks, tu_blocks, tv_blocks, facet_blocks, u_blocks, v_blocks))
    plane = grid[0] + 1j * grid[1]
    picture = jnp.fft.ifft2(plane) * (float(GRID) * float(GRID) / jnp.sqrt(float(VISIBILITIES)))
    return jnp.stack([jnp.real(picture), jnp.imag(picture)]).astype(jnp.float32)
```

```python
import functools
import math

import jax
import jax.numpy as jnp
import numpy as np
from jax import lax
from jax.experimental import pallas as pl
from jax.experimental.pallas import tpu as pltpu
from jax.sharding import PartitionSpec as P

GRID = 8192
TAPS = 16
LANES = 128
LOW = 128
FIELDS = 40
WINDOW_BLOCKS = 2
ROWS_OUT = 8
MEBI = 1024 * 1024


def phase_table(left, right, modulus):
    product = left[:, None] * right[None, :] % modulus
    angle = product.astype(jnp.float32) * (2.0 * math.pi / modulus)
    return jnp.cos(angle), jnp.sin(angle)


def rotated(taps, shift):
    tap = jnp.arange(TAPS, dtype=jnp.int32)[:, None]
    turned = jnp.zeros_like(taps)
    for t in range(TAPS):
        turned = turned + jnp.where((shift[None, :] + t) % TAPS == tap, taps[t : t + 1], 0)
    return turned


def spread_tile(fields, low_ref, high_ref, period):
    tile = fields.shape[1]
    taps_u = fields[TAPS : 2 * TAPS]
    extra = fields[2 * TAPS : 2 * TAPS + 8].astype(jnp.float32)
    row_high = extra[3:4].astype(jnp.bfloat16)
    row_mid = extra[4:5]
    row_low = extra[5:6]
    vis_re = extra[6:7].astype(jnp.bfloat16)
    vis_im = extra[7:8].astype(jnp.bfloat16)
    zero = jnp.zeros((), jnp.bfloat16)
    tap = lax.broadcasted_iota(jnp.int32, (TAPS, tile), 0).astype(jnp.float32)
    spot_u = (row_mid + jnp.where(tap < row_low, 1.0, 0.0)).astype(jnp.bfloat16)
    band_u = jnp.concatenate(
        [jnp.where(spot_u == jnp.bfloat16(q), taps_u, zero) for q in range(LOW // TAPS + 1)], axis=0
    )
    high_count = GRID // LOW
    number = lax.broadcasted_iota(jnp.int32, (high_count, tile), 0).astype(jnp.float32).astype(jnp.bfloat16)
    here = number == jnp.broadcast_to(row_high, (high_count, tile))
    picked = jnp.concatenate(
        [
            jnp.where(here, jnp.broadcast_to(vis_re, (high_count, tile)), zero),
            jnp.where(here, jnp.broadcast_to(vis_im, (high_count, tile)), zero),
        ],
        axis=0,
    )
    high = jnp.dot(high_ref[...], picked, preferred_element_type=jnp.float32)
    high_re, high_im = high[:period], high[period:]
    low = jnp.dot(low_ref[...], band_u, preferred_element_type=jnp.float32)
    parts = []
    for begin in range(0, low.shape[0], 2 * period):
        low_re = low[begin : begin + period]
        low_im = low[begin + period : begin + 2 * period]
        parts.append((low_re * high_re - low_im * high_im).astype(jnp.bfloat16))
        parts.append((low_re * high_im + low_im * high_re).astype(jnp.bfloat16))
    return jnp.concatenate(parts, axis=0)


def add_window(spread, fields, block, acc_ref):
    tile = fields.shape[1]
    taps_v = fields[0:TAPS]
    extra = fields[2 * TAPS : 2 * TAPS + 8].astype(jnp.float32)
    tap = lax.broadcasted_iota(jnp.int32, (TAPS, tile), 0).astype(jnp.float32)
    groups = LANES // TAPS
    count = WINDOW_BLOCKS * groups
    zero = jnp.zeros((), jnp.bfloat16)
    spot = (extra[0:1] - block.astype(jnp.float32)) * groups + extra[1:2] + jnp.where(tap < extra[2:3], 1.0, 0.0)
    near = jnp.clip(spot, -1.0, float(count)).astype(jnp.bfloat16)
    band_v = jnp.concatenate([jnp.where(near == jnp.bfloat16(q), taps_v, zero) for q in range(count)], axis=0)
    out = lax.dot_general(spread, band_v, (((1,), (1,)), ((), ())), preferred_element_type=jnp.float32)
    for j in range(WINDOW_BLOCKS):
        acc_ref[block + j] += out[:, j * LANES : (j + 1) * LANES]


def image_kernel(
    first_ref, extra_ref, pay_ref, low_ref, high_ref, one_ref, cos_ref, sin_ref, two_ref, out_ref, acc_ref, *spreads,
    tile, tiles, lists, period,
):
    step = pl.program_id(0)
    group = len(spreads)
    blocks = GRID // LANES

    @pl.when(step == 0)
    def _():
        def clear(n, carry):
            acc_ref[n] = jnp.zeros(acc_ref.shape[1:], jnp.float32)
            return carry

        lax.fori_loop(0, acc_ref.shape[0], clear, 0)

    @pl.when(step < lists)
    def _():
        def some_tiles(g, carry):
            start = g * group
            place = step * tiles + start
            fields = lambda n: pay_ref[0, :, pl.ds(pl.multiple_of((start + n) * tile, tile), tile)]
            for n in range(group):
                spread = spread_tile(fields(n), low_ref, high_ref, period)
                spreads[n][...] = spread
                add_window(spread, fields(n), first_ref[place + n], acc_ref)
            for n in range(group):
                def more(window, carry, n=n):
                    block = jnp.minimum(first_ref[place + n] + window * WINDOW_BLOCKS, blocks)
                    add_window(spreads[n][...], fields(n), block, acc_ref)
                    return carry

                lax.fori_loop(1, extra_ref[place + n], more, 0)
            return carry

        lax.fori_loop(0, tiles // group, some_tiles, 0)

    @pl.when(step >= lists)
    def _():
        first_row = (step - lists) * ROWS_OUT
        at = first_row // period * (2 * period) + first_row % period
        read = lambda part: acc_ref[0:blocks, pl.ds(pl.multiple_of(at + part * period, ROWS_OUT), ROWS_OUT), :]
        planes = [read(0), read(1)]
        stack = jnp.concatenate(
            [jnp.concatenate([plane[:, m, :] for m in range(ROWS_OUT)], axis=1) for plane in planes], axis=0
        ).astype(jnp.bfloat16)
        mid = jnp.dot(one_ref[...], stack, preferred_element_type=jnp.float32)
        cos, sin = cos_ref[...], sin_ref[...]
        rows = []
        for m in range(ROWS_OUT):
            re = mid[:blocks, m * LANES : (m + 1) * LANES]
            im = mid[blocks:, m * LANES : (m + 1) * LANES]
            rows.append(
                jnp.concatenate(
                    [(re * cos - im * sin).astype(jnp.bfloat16), (re * sin + im * cos).astype(jnp.bfloat16)], axis=1
                )
            )
        turned = jnp.concatenate(rows, axis=0)
        out = lax.dot_general(two_ref[...], turned, (((1,), (1,)), ((), ())), preferred_element_type=jnp.float32)
        half = LANES // 2
        left = lax.broadcasted_iota(jnp.int32, (half, LANES), 1) < half
        for part in range(2):
            for pair in range(ROWS_OUT // 2):
                lanes = slice(pair * LANES, (pair + 1) * LANES)
                even = out[2 * part * half : (2 * part + 1) * half, lanes]
                odd = out[(2 * part + 1) * half : (2 * part + 2) * half, lanes]
                out_ref[part, 0, pl.ds(2 * pair, blocks, stride=ROWS_OUT), :] = jnp.where(left, even, pltpu.roll(odd, half, 1))
                out_ref[part, 0, pl.ds(2 * pair + 1, blocks, stride=ROWS_OUT), :] = jnp.where(
                    left, pltpu.roll(even, half, 1), odd
                )

MESH = pl.DeviceIdType.MESH


def exchange_kernel(src_ref, dst_ref, send_sem, recv_sem, *, axis):
    size = send_sem.shape[0]
    me = lax.rem(lax.axis_index(axis), size)
    base = lax.axis_index(axis) - me
    width = src_ref.shape[1] // size
    barrier = pltpu.get_barrier_semaphore()
    for hop in range(1, size):
        peer = base + lax.rem(me + hop, size)
        pl.semaphore_signal(barrier, inc=1, device_id={axis: peer}, device_id_type=MESH)
    pl.semaphore_wait(barrier, size - 1)
    piece = lambda ref, n: ref.at[:, pl.ds(pl.multiple_of(n * width, width), width)]
    copies = []
    for hop in range(1, size):
        peer = lax.rem(me + hop, size)
        copy = pltpu.make_async_remote_copy(
            src_ref=piece(src_ref, peer),
            dst_ref=piece(dst_ref, me),
            send_sem=send_sem.at[hop],
            recv_sem=recv_sem.at[hop],
            device_id={axis: base + peer},
            device_id_type=MESH,
        )
        copy.start()
        copies.append(copy)
    own = pltpu.make_async_copy(piece(src_ref, me), piece(dst_ref, me), send_sem.at[0])
    own.start()
    own.wait()
    for copy in copies:
        copy.wait()


def exchanged(payload, axis, number):
    size = math.gcd(lax.axis_size(axis), payload.shape[1] // LANES)
    return pl.pallas_call(
        functools.partial(exchange_kernel, axis=axis),
        in_specs=[pl.BlockSpec(memory_space=pltpu.HBM)],
        out_specs=pl.BlockSpec(memory_space=pltpu.HBM),
        out_shape=jax.ShapeDtypeStruct(payload.shape, payload.dtype),
        scratch_shapes=[pltpu.SemaphoreType.DMA((size,)), pltpu.SemaphoreType.DMA((size,))],
        compiler_params=pltpu.CompilerParams(collective_id=number, has_side_effects=True),
    )(payload)


def gather_kernel(src_ref, out_ref, own_sem, send_sem, recv_sem):
    n_au, n_vert = lax.axis_size("au"), lax.axis_size("vert")
    a, v = lax.axis_index("au"), lax.axis_index("vert")
    width = out_ref.shape[3]
    inner, cores = math.gcd(n_au, 2), math.gcd(n_vert, 2)
    sizes = {"x": inner, "y": n_au // inner, "z": n_vert // cores, "c": cores}
    place = {"x": lax.rem(a, inner), "y": a // inner, "z": v // cores, "c": lax.rem(v, cores)}

    def at(**moved):
        spot = dict(place)
        for name, hop in moved.items():
            spot[name] = lax.rem(place[name] + hop, sizes[name]) if hop else place[name]
        return spot["y"] * inner + spot["x"], spot["z"] * cores + spot["c"]

    steps = [(name, hop) for name in "xyzc" for hop in range(1, sizes[name])]
    barrier = pltpu.get_barrier_semaphore()
    for name, hop in steps:
        au, vert = at(**{name: hop})
        pl.semaphore_signal(barrier, inc=1, device_id={"au": au, "vert": vert}, device_id_type=MESH)
    pl.semaphore_wait(barrier, len(steps))

    sent = []

    def send(half, source, moved, name, hop):
        au, vert = at(**moved)
        origin = au * n_vert + vert
        to_au, to_vert = at(**{name: hop})
        path = dict(moved)
        path[name] = -hop
        slot = tuple(path.get(n, 0) % sizes[n] for n in "xyzc")
        copy = pltpu.make_async_remote_copy(
            src_ref=source,
            dst_ref=out_ref.at[origin, half],
            send_sem=send_sem.at[len(sent)],
            recv_sem=recv_sem.at[number(half, slot)],
            device_id={"au": to_au, "vert": to_vert},
            device_id_type=MESH,
        )
        copy.start()
        sent.append(copy)

    def number(half, slot):
        total = half
        for n, d in zip("xyzc", slot):
            total = total * sizes[n] + d
        return total

    def arrived(half, moved):
        au, vert = at(**moved)
        block = out_ref.at[au * n_vert + vert, half]
        slot = tuple(moved.get(n, 0) for n in "xyzc")
        pltpu.make_async_copy(block, block, recv_sem.at[number(half, slot)]).wait()
        return block

    order = [("z", "x", "y", "c"), ("z", "y", "x", "c")]

    def pass_on(half, source, moved, stage):
        for name in order[half][stage:]:
            for hop in range(1, sizes[name]):
                send(half, source, moved, name, hop)

    halves = [src_ref.at[:, pl.ds(h * width, width)] for h in range(2)]
    for half in range(2):
        pass_on(half, halves[half], {}, 0)
    origin = a * n_vert + v
    keep = [pltpu.make_async_copy(halves[h], out_ref.at[origin, h], own_sem.at[h]) for h in range(2)]
    for copy in keep:
        copy.start()
    last = []
    for hop_z in range(sizes["z"]):
        for half in range(2):
            if hop_z:
                pass_on(half, arrived(half, {"z": hop_z}), {"z": hop_z}, 1)
        for half in range(2):
            second = order[half][1]
            for hop in range(1, sizes[second]):
                moved = {"z": hop_z, second: hop}
                pass_on(half, arrived(half, moved), moved, 2)
    for hop_z in range(sizes["z"]):
        for half in range(2):
            second, third = order[half][1:3]
            for hop in range(sizes[second]):
                for hop_third in range(1, sizes[third]):
                    moved = {"z": hop_z, second: hop, third: hop_third}
                    pass_on(half, arrived(half, moved), moved, 3)
    for half in range(2):
        for hop in range(1, sizes["c"]):
            for x in range(sizes["x"]):
                for y in range(sizes["y"]):
                    for z in range(sizes["z"]):
                        arrived(half, {"c": hop, "x": x, "y": y, "z": z})
    for copy in keep:
        copy.wait()
    for copy in sent:
        copy.wait_send()


def gathered_everywhere(payload, devices, number):
    fields, count = payload.shape
    return pl.pallas_call(
        gather_kernel,
        in_specs=[pl.BlockSpec(memory_space=pltpu.VMEM)],
        out_specs=pl.BlockSpec(memory_space=pltpu.HBM),
        out_shape=jax.ShapeDtypeStruct((devices, 2, fields, count // 2), payload.dtype),
        scratch_shapes=[
            pltpu.SemaphoreType.DMA((2,)),
            pltpu.SemaphoreType.DMA((2 * devices,)),
            pltpu.SemaphoreType.DMA((2 * devices,)),
        ],
        compiler_params=pltpu.CompilerParams(collective_id=number, has_side_effects=True),
    )(payload)


def fixed_table(left, right, modulus):
    angle = np.outer(left, right) % modulus * (2.0 * math.pi / modulus)
    return np.cos(angle), np.sin(angle)


def stacked(cos, sin):
    return jnp.asarray(np.block([[cos, -sin], [sin, cos]]), dtype=jnp.bfloat16)


def columns_of(payload):
    ends = payload[..., 2 * TAPS : 2 * TAPS + 3, :].astype(jnp.int32)
    return ends[..., 0, :] * LANES + ends[..., 1, :] * TAPS + ends[..., 2, :]


def ordered(payload):
    count = payload.shape[1]
    key = columns_of(payload) * count + jnp.arange(count, dtype=jnp.int32)
    rank = jnp.sum((key[:, None] < key[None, :]).astype(jnp.int32), axis=0)
    order = (rank[:, None] == jnp.arange(count, dtype=jnp.int32)[None, :]).astype(jnp.bfloat16)
    return jnp.dot(payload, order, preferred_element_type=jnp.float32).astype(jnp.bfloat16)


def on_device(visibility, taps_u, taps_v, facet, u_offset, v_offset):
    n_au = lax.axis_size("au")
    n_vert = lax.axis_size("vert")
    devices = n_au * n_vert
    count = visibility.shape[1]
    rows = GRID // devices
    own = lax.axis_index("au") * n_vert + lax.axis_index("vert")
    target = facet[:, 0]
    row = target // n_vert * (GRID // n_au) + u_offset
    col = target % n_vert * (GRID // n_vert) + v_offset
    scalars = jnp.stack(
        [col // LANES, col % LANES // TAPS, col % TAPS, row // LOW, row % LOW // TAPS, row % TAPS]
    ).astype(jnp.bfloat16)
    payload = jnp.concatenate(
        [rotated(taps_v, col % TAPS), rotated(taps_u, row % TAPS), scalars, visibility], axis=0
    )
    payload = ordered(payload)
    payload = exchanged(payload, "vert", 0)
    payload = ordered(payload)
    payload = exchanged(payload, "au", 1)
    payload = ordered(payload)
    lists, count = 2 * devices, count // 2
    gathered = gathered_everywhere(payload, devices, 2).reshape(lists, FIELDS, count)

    tile = math.gcd(count, 256)
    tiles = count // tile
    blocks = GRID // LANES
    columns = columns_of(gathered).reshape(-1, tile)
    first = jnp.min(columns, axis=1) // LANES
    windows = ((jnp.max(columns, axis=1) + TAPS - 1) // LANES - first) // WINDOW_BLOCKS + 1

    k = own * rows + jnp.arange(rows, dtype=jnp.int32)
    high_count = GRID // LOW
    period = min(rows, high_count)
    low_cos, low_sin = phase_table(k, jnp.arange(LOW + TAPS, dtype=jnp.int32), GRID)
    low_table = jnp.concatenate(
        [low_cos.reshape(rows // period, 1, period, -1), low_sin.reshape(rows // period, 1, period, -1)], axis=1
    ).reshape(2 * rows, -1).astype(jnp.bfloat16)
    turns = phase_table(k[:period], jnp.arange(high_count, dtype=jnp.int32), high_count)
    high_table = jnp.block([[turns[0], -turns[1]], [turns[1], turns[0]]]).astype(jnp.bfloat16)

    a, b = np.arange(blocks), np.arange(LANES)
    one_table = stacked(*fixed_table(a, a, blocks))
    cos, sin = fixed_table(a, b, GRID)
    scale = 1.0 / math.sqrt(count * lists)
    mu = np.concatenate([np.arange(0, LANES, 2), np.arange(1, LANES, 2)])
    two_table = stacked(*fixed_table(mu, b, LANES))
    cos, sin = jnp.asarray(cos * scale, dtype=jnp.float32), jnp.asarray(sin * scale, dtype=jnp.float32)
    whole = lambda shape: pl.BlockSpec(shape, lambda n, *_: (0,) * len(shape))
    group = math.gcd(tiles, 4)
    picture = pl.pallas_call(
        functools.partial(image_kernel, tile=tile, tiles=tiles, lists=lists, period=period),
        grid_spec=pltpu.PrefetchScalarGridSpec(
            num_scalar_prefetch=2,
            grid=(lists + rows // ROWS_OUT,),
            in_specs=[
                pl.BlockSpec((1, FIELDS, count), lambda s, *_: (jnp.minimum(s, lists - 1), 0, 0)),
                whole(low_table.shape),
                whole(high_table.shape),
                whole(one_table.shape),
                whole(cos.shape),
                whole(sin.shape),
                whole(two_table.shape),
            ],
            out_specs=pl.BlockSpec(
                (2, 1, blocks * ROWS_OUT, LANES), lambda s, *_: (0, jnp.maximum(s - lists, 0), 0, 0)
            ),
            scratch_shapes=[pltpu.VMEM((blocks + WINDOW_BLOCKS, 2 * rows, LANES), jnp.float32)]
            + [pltpu.VMEM((2 * rows, tile), jnp.bfloat16)] * group,
        ),
        out_shape=jax.ShapeDtypeStruct((2, rows // ROWS_OUT, blocks * ROWS_OUT, LANES), jnp.float32),
        compiler_params=pltpu.CompilerParams(vmem_limit_bytes=56 * MEBI),
    )(first, windows, gathered, low_table, high_table, one_table, cos, sin, two_table)
    picture = picture.reshape(2, rows // ROWS_OUT, blocks, ROWS_OUT, LANES)
    return jnp.transpose(picture, (0, 1, 3, 2, 4)).reshape(2, rows, GRID)


def solution(mesh):
    return jax.shard_map(
        on_device,
        mesh=mesh,
        in_specs=(
            P(None, ("au", "vert")),
            P(None, ("au", "vert")),
            P(None, ("au", "vert")),
            P(("au", "vert"), None),
            P(("au", "vert")),
            P(("au", "vert")),
        ),
        out_specs=P(None, ("au", "vert"), None),
        check_vma=False,
    )
```

```python
import functools
import math

import jax
import jax.numpy as jnp
import numpy as np
from jax import lax
from jax.experimental import pallas as pl
from jax.experimental.pallas import tpu as pltpu
from jax.sharding import PartitionSpec as P

GRID = 8192
TAPS = 16
LANES = 128
LOW = 128
FIELDS = 40
WINDOW_BLOCKS = 2
ROWS_OUT = 8
OUT_GROUPS = 2
PAD = 8
MEBI = 1024 * 1024


def phase_table(left, right, modulus):
    product = left[:, None] * right[None, :] % modulus
    angle = product.astype(jnp.float32) * (2.0 * math.pi / modulus)
    return jnp.cos(angle), jnp.sin(angle)


def rotated(taps, shift):
    tap = jnp.arange(TAPS, dtype=jnp.int32)[:, None]
    turned = jnp.zeros_like(taps)
    for t in range(TAPS):
        turned = turned + jnp.where((shift[None, :] + t) % TAPS == tap, taps[t : t + 1], 0)
    return turned


def spread_tile(fields, low_ref, high_ref, period):
    tile = fields.shape[1]
    taps_u = fields[TAPS : 2 * TAPS]
    extra = fields[2 * TAPS : 2 * TAPS + 8].astype(jnp.float32)
    row_high = extra[3:4].astype(jnp.bfloat16)
    row_mid = extra[4:5]
    row_low = extra[5:6]
    vis_re = extra[6:7].astype(jnp.bfloat16)
    vis_im = extra[7:8].astype(jnp.bfloat16)
    zero = jnp.zeros((), jnp.bfloat16)
    tap = lax.broadcasted_iota(jnp.int32, (TAPS, tile), 0).astype(jnp.float32)
    spot_u = (row_mid + jnp.where(tap < row_low, 1.0, 0.0)).astype(jnp.bfloat16)
    band_u = jnp.concatenate(
        [jnp.where(spot_u == jnp.bfloat16(q), taps_u, zero) for q in range(LOW // TAPS + 1)], axis=0
    )
    high_count = GRID // LOW
    number = lax.broadcasted_iota(jnp.int32, (high_count, tile), 0).astype(jnp.float32).astype(jnp.bfloat16)
    here = number == jnp.broadcast_to(row_high, (high_count, tile))
    picked = jnp.concatenate(
        [
            jnp.where(here, jnp.broadcast_to(vis_re, (high_count, tile)), zero),
            jnp.where(here, jnp.broadcast_to(vis_im, (high_count, tile)), zero),
        ],
        axis=0,
    )
    high = jnp.dot(high_ref[...], picked, preferred_element_type=jnp.float32)
    high_re, high_im = high[:period], high[period:]
    low = jnp.dot(low_ref[...], band_u, preferred_element_type=jnp.float32)
    parts = []
    for begin in range(0, low.shape[0], 2 * period):
        low_re = low[begin : begin + period]
        low_im = low[begin + period : begin + 2 * period]
        parts.append((low_re * high_re - low_im * high_im).astype(jnp.bfloat16))
        parts.append((low_re * high_im + low_im * high_re).astype(jnp.bfloat16))
    return jnp.concatenate(parts, axis=0)


def add_window(spread, fields, block, acc_ref):
    tile = fields.shape[1]
    taps_v = fields[0:TAPS]
    extra = fields[2 * TAPS : 2 * TAPS + 8].astype(jnp.float32)
    tap = lax.broadcasted_iota(jnp.int32, (TAPS, tile), 0).astype(jnp.float32)
    groups = LANES // TAPS
    count = WINDOW_BLOCKS * groups
    zero = jnp.zeros((), jnp.bfloat16)
    spot = (extra[0:1] - block.astype(jnp.float32)) * groups + extra[1:2] + jnp.where(tap < extra[2:3], 1.0, 0.0)
    near = jnp.clip(spot, -1.0, float(count)).astype(jnp.bfloat16)
    band_v = jnp.concatenate([jnp.where(near == jnp.bfloat16(q), taps_v, zero) for q in range(count)], axis=0)
    out = lax.dot_general(spread, band_v, (((1,), (1,)), ((), ())), preferred_element_type=jnp.float32)
    pitch = spread.shape[0] + PAD
    for j in range(WINDOW_BLOCKS):
        rows = pl.ds(pl.multiple_of((block + j) * pitch, PAD), spread.shape[0])
        acc_ref[rows, :] += out[:, j * LANES : (j + 1) * LANES]


def image_kernel(
    first_ref, extra_ref, pay_ref, low_ref, high_ref, one_ref, cos_ref, sin_ref, two_ref, out_ref, acc_ref, *spreads,
    tile, tiles, lists, period,
):
    step = pl.program_id(0)
    blocks = GRID // LANES
    pitch = low_ref.shape[0] + PAD

    @pl.when(step == 0)
    def _():
        def clear(n, carry):
            rows = pl.ds(pl.multiple_of(n * pitch, PAD), pitch)
            acc_ref[rows, :] = jnp.zeros((pitch, LANES), jnp.float32)
            return carry

        lax.fori_loop(0, acc_ref.shape[0] // pitch, clear, 0)

    @pl.when(step < lists)
    def _():
        def one_list(part, carry):
            place = (step * pay_ref.shape[0] + part) * 2 * tiles
            fields = lambda n: pay_ref[part, n // tiles, :, n % tiles * tile : (n % tiles + 1) * tile]
            for n in range(2 * tiles):
                spread = spread_tile(fields(n), low_ref, high_ref, period)
                spreads[n][...] = spread
                add_window(spread, fields(n), first_ref[place + n], acc_ref)
            for n in range(2 * tiles):
                def more(window, carry, n=n):
                    block = jnp.minimum(first_ref[place + n] + window * WINDOW_BLOCKS, blocks)
                    add_window(spreads[n][...], fields(n), block, acc_ref)
                    return carry

                lax.fori_loop(1, extra_ref[place + n], more, 0)
            return carry

        lax.fori_loop(0, pay_ref.shape[0], one_list, 0)

    @pl.when(step >= lists)
    def _():
        def some_rows(turn, carry):
            for group in range(OUT_GROUPS):
                here = turn * OUT_GROUPS + group
                first_row = ((step - lists) * out_ref.shape[1] + here) * ROWS_OUT
                at = first_row // period * (2 * period) + first_row % period
                image_rows(at, period, acc_ref, one_ref, cos_ref, sin_ref, two_ref, out_ref, here, pitch)
            return carry

        lax.fori_loop(0, out_ref.shape[1] // OUT_GROUPS, some_rows, 0)


def image_rows(at, period, acc_ref, one_ref, cos_ref, sin_ref, two_ref, out_ref, group, pitch):
    blocks = GRID // LANES
    row = lambda part, m: acc_ref[pl.ds(at + part * period + m, blocks, stride=pitch), :].astype(jnp.bfloat16)
    stack = jnp.concatenate(
        [jnp.concatenate([row(part, m) for m in range(ROWS_OUT)], axis=1) for part in range(2)], axis=0
    )
    mid = jnp.dot(one_ref[...], stack, preferred_element_type=jnp.float32)
    cos, sin = cos_ref[...], sin_ref[...]
    rows = []
    for m in range(ROWS_OUT):
        re = mid[:blocks, m * LANES : (m + 1) * LANES]
        im = mid[blocks:, m * LANES : (m + 1) * LANES]
        rows.append(
            jnp.concatenate(
                [(re * cos - im * sin).astype(jnp.bfloat16), (re * sin + im * cos).astype(jnp.bfloat16)], axis=1
            )
        )
    turned = jnp.concatenate(rows, axis=0)
    out = lax.dot_general(two_ref[...], turned, (((1,), (1,)), ((), ())), preferred_element_type=jnp.float32)
    half = LANES // 2
    left = lax.broadcasted_iota(jnp.int32, (half, LANES), 1) < half
    for part in range(2):
        for pair in range(ROWS_OUT // 2):
            lanes = slice(pair * LANES, (pair + 1) * LANES)
            even = out[2 * part * half : (2 * part + 1) * half, lanes]
            odd = out[(2 * part + 1) * half : (2 * part + 2) * half, lanes]
            put = lambda m: pl.ds(m, blocks, stride=ROWS_OUT)
            out_ref[part, group, put(2 * pair), :] = jnp.where(left, even, pltpu.roll(odd, half, 1))
            out_ref[part, group, put(2 * pair + 1), :] = jnp.where(left, pltpu.roll(even, half, 1), odd)


MESH = pl.DeviceIdType.MESH


def exchange_kernel(src_ref, dst_ref, send_sem, recv_sem, *, sizes):
    spot, near, me = {}, {}, 0
    for axis, size in sizes.items():
        near[axis] = lax.rem(lax.axis_index(axis), size)
        spot[axis] = lax.axis_index(axis) - near[axis]
        me = me * size + near[axis]
    total = math.prod(sizes.values())
    width = src_ref.shape[1] // total

    def peer(hop):
        index, device = 0, {}
        for place, (axis, size) in enumerate(sizes.items()):
            step = hop // math.prod(list(sizes.values())[place + 1 :]) % size
            digit = lax.rem(near[axis] + step, size) if step else near[axis]
            index = index * size + digit
            device[axis] = spot[axis] + digit
        return index, device

    barrier = pltpu.get_barrier_semaphore()
    for hop in range(1, total):
        pl.semaphore_signal(barrier, inc=1, device_id=peer(hop)[1], device_id_type=MESH)
    pl.semaphore_wait(barrier, total - 1)
    piece = lambda ref, n: ref.at[:, pl.ds(pl.multiple_of(n * width, width), width)]
    copies = []
    for hop in range(1, total):
        index, device = peer(hop)
        copy = pltpu.make_async_remote_copy(
            src_ref=piece(src_ref, index),
            dst_ref=piece(dst_ref, me),
            send_sem=send_sem.at[hop],
            recv_sem=recv_sem.at[hop],
            device_id=device,
            device_id_type=MESH,
        )
        copy.start()
        copies.append(copy)
    own = pltpu.make_async_copy(piece(src_ref, me), piece(dst_ref, me), send_sem.at[0])
    own.start()
    own.wait()
    for copy in copies:
        copy.wait()


def exchanged(payload, number):
    vert = math.gcd(lax.axis_size("vert"), payload.shape[1] // LANES)
    sizes = {"au": math.gcd(lax.axis_size("au"), payload.shape[1] // LANES // vert), "vert": vert}
    total = math.prod(sizes.values())
    return pl.pallas_call(
        functools.partial(exchange_kernel, sizes=sizes),
        in_specs=[pl.BlockSpec(memory_space=pltpu.HBM)],
        out_specs=pl.BlockSpec(memory_space=pltpu.HBM),
        out_shape=jax.ShapeDtypeStruct(payload.shape, payload.dtype),
        scratch_shapes=[pltpu.SemaphoreType.DMA((total,)), pltpu.SemaphoreType.DMA((total,))],
        compiler_params=pltpu.CompilerParams(collective_id=number, has_side_effects=True),
    )(payload)


def gather_kernel(src_ref, out_ref, own_sem, send_sem, recv_sem):
    n_au, n_vert = lax.axis_size("au"), lax.axis_size("vert")
    a, v = lax.axis_index("au"), lax.axis_index("vert")
    width = out_ref.shape[3]
    inner, cores = math.gcd(n_au, 2), math.gcd(n_vert, 2)
    sizes = {"x": inner, "y": n_au // inner, "z": n_vert // cores, "c": cores}
    place = {"x": lax.rem(a, inner), "y": a // inner, "z": v // cores, "c": lax.rem(v, cores)}

    def at(**moved):
        spot = dict(place)
        for name, hop in moved.items():
            spot[name] = lax.rem(place[name] + hop, sizes[name]) if hop else place[name]
        return spot["y"] * inner + spot["x"], spot["z"] * cores + spot["c"]

    steps = [(name, hop) for name in "xyzc" for hop in range(1, sizes[name])]
    barrier = pltpu.get_barrier_semaphore()
    for name, hop in steps:
        au, vert = at(**{name: hop})
        pl.semaphore_signal(barrier, inc=1, device_id={"au": au, "vert": vert}, device_id_type=MESH)
    pl.semaphore_wait(barrier, len(steps))

    sent = []

    def send(half, source, moved, name, hop):
        au, vert = at(**moved)
        origin = au * n_vert + vert
        to_au, to_vert = at(**{name: hop})
        path = dict(moved)
        path[name] = -hop
        slot = tuple(path.get(n, 0) % sizes[n] for n in "xyzc")
        copy = pltpu.make_async_remote_copy(
            src_ref=source,
            dst_ref=out_ref.at[origin, half],
            send_sem=send_sem.at[len(sent)],
            recv_sem=recv_sem.at[number(half, slot)],
            device_id={"au": to_au, "vert": to_vert},
            device_id_type=MESH,
        )
        copy.start()
        sent.append(copy)

    def number(half, slot):
        total = half
        for n, d in zip("xyzc", slot):
            total = total * sizes[n] + d
        return total

    def arrived(half, moved):
        au, vert = at(**moved)
        block = out_ref.at[au * n_vert + vert, half]
        slot = tuple(moved.get(n, 0) for n in "xyzc")
        pltpu.make_async_copy(block, block, recv_sem.at[number(half, slot)]).wait()
        return block

    order = [("z", "x", "y", "c"), ("z", "y", "x", "c")]

    def pass_on(half, source, moved, stage):
        for name in order[half][stage:]:
            for hop in range(1, sizes[name]):
                send(half, source, moved, name, hop)

    halves = [src_ref.at[:, pl.ds(h * width, width)] for h in range(2)]
    for half in range(2):
        pass_on(half, halves[half], {}, 0)
    origin = a * n_vert + v
    keep = [pltpu.make_async_copy(halves[h], out_ref.at[origin, h], own_sem.at[h]) for h in range(2)]
    for copy in keep:
        copy.start()
    last = []
    for hop_z in range(sizes["z"]):
        for half in range(2):
            if hop_z:
                pass_on(half, arrived(half, {"z": hop_z}), {"z": hop_z}, 1)
        for half in range(2):
            second = order[half][1]
            for hop in range(1, sizes[second]):
                moved = {"z": hop_z, second: hop}
                pass_on(half, arrived(half, moved), moved, 2)
    for hop_z in range(sizes["z"]):
        for half in range(2):
            second, third = order[half][1:3]
            for hop in range(sizes[second]):
                for hop_third in range(1, sizes[third]):
                    moved = {"z": hop_z, second: hop, third: hop_third}
                    pass_on(half, arrived(half, moved), moved, 3)
    for half in range(2):
        for hop in range(1, sizes["c"]):
            for x in range(sizes["x"]):
                for y in range(sizes["y"]):
                    for z in range(sizes["z"]):
                        arrived(half, {"c": hop, "x": x, "y": y, "z": z})
    for copy in keep:
        copy.wait()
    for copy in sent:
        copy.wait_send()


def gathered_everywhere(payload, devices, number):
    fields, count = payload.shape
    return pl.pallas_call(
        gather_kernel,
        in_specs=[pl.BlockSpec(memory_space=pltpu.VMEM)],
        out_specs=pl.BlockSpec(memory_space=pltpu.HBM),
        out_shape=jax.ShapeDtypeStruct((devices, 2, fields, count // 2), payload.dtype),
        scratch_shapes=[
            pltpu.SemaphoreType.DMA((2,)),
            pltpu.SemaphoreType.DMA((2 * devices,)),
            pltpu.SemaphoreType.DMA((2 * devices,)),
        ],
        compiler_params=pltpu.CompilerParams(collective_id=number, has_side_effects=True),
    )(payload)


def fixed_table(left, right, modulus):
    angle = np.outer(left, right) % modulus * (2.0 * math.pi / modulus)
    return np.cos(angle), np.sin(angle)


def stacked(cos, sin):
    return jnp.asarray(np.block([[cos, -sin], [sin, cos]]), dtype=jnp.bfloat16)


def columns_of(payload):
    ends = payload[..., 2 * TAPS : 2 * TAPS + 3, :].astype(jnp.int32)
    return ends[..., 0, :] * LANES + ends[..., 1, :] * TAPS + ends[..., 2, :]


def ordered(payload):
    count = payload.shape[1]
    key = columns_of(payload) * count + jnp.arange(count, dtype=jnp.int32)
    rank = jnp.sum((key[:, None] < key[None, :]).astype(jnp.int32), axis=0)
    order = (rank[:, None] == jnp.arange(count, dtype=jnp.int32)[None, :]).astype(jnp.bfloat16)
    return jnp.dot(payload, order, preferred_element_type=jnp.float32).astype(jnp.bfloat16)


def on_device(visibility, taps_u, taps_v, facet, u_offset, v_offset):
    n_au = lax.axis_size("au")
    n_vert = lax.axis_size("vert")
    devices = n_au * n_vert
    count = visibility.shape[1]
    rows = GRID // devices
    own = lax.axis_index("au") * n_vert + lax.axis_index("vert")
    target = facet[:, 0]
    row = target // n_vert * (GRID // n_au) + u_offset
    col = target % n_vert * (GRID // n_vert) + v_offset
    scalars = jnp.stack(
        [col // LANES, col % LANES // TAPS, col % TAPS, row // LOW, row % LOW // TAPS, row % TAPS]
    ).astype(jnp.bfloat16)
    payload = jnp.concatenate(
        [rotated(taps_v, col % TAPS), rotated(taps_u, row % TAPS), scalars, visibility], axis=0
    )
    payload = ordered(payload)
    payload = exchanged(payload, 0)
    payload = ordered(payload)
    gathered = gathered_everywhere(payload, devices, 1)
    tile = math.gcd(count // 2, 256)
    tiles = count // 2 // tile
    blocks = GRID // LANES
    columns = columns_of(gathered).reshape(-1, tile)
    first = jnp.min(columns, axis=1) // LANES
    windows = ((jnp.max(columns, axis=1) + TAPS - 1) // LANES - first) // WINDOW_BLOCKS + 1

    k = own * rows + jnp.arange(rows, dtype=jnp.int32)
    high_count = GRID // LOW
    period = min(rows, high_count)
    low_cos, low_sin = phase_table(k, jnp.arange(LOW + TAPS, dtype=jnp.int32), GRID)
    low_table = jnp.concatenate(
        [low_cos.reshape(rows // period, 1, period, -1), low_sin.reshape(rows // period, 1, period, -1)], axis=1
    ).reshape(2 * rows, -1).astype(jnp.bfloat16)
    turns = phase_table(k[:period], jnp.arange(high_count, dtype=jnp.int32), high_count)
    high_table = jnp.block([[turns[0], -turns[1]], [turns[1], turns[0]]]).astype(jnp.bfloat16)

    a, b = np.arange(blocks), np.arange(LANES)
    one_table = stacked(*fixed_table(a, a, blocks))
    cos, sin = fixed_table(a, b, GRID)
    scale = 1.0 / math.sqrt(count * devices)
    mu = np.concatenate([np.arange(0, LANES, 2), np.arange(1, LANES, 2)])
    two_table = stacked(*fixed_table(mu, b, LANES))
    cos, sin = jnp.asarray(cos * scale, dtype=jnp.float32), jnp.asarray(sin * scale, dtype=jnp.float32)
    together = math.gcd(devices, 4)
    steps = devices // together
    out_rows = OUT_GROUPS * math.gcd(rows // (ROWS_OUT * OUT_GROUPS), 2)
    whole = lambda shape: pl.BlockSpec(shape, lambda n, *_: (0,) * len(shape))
    picture = pl.pallas_call(
        functools.partial(image_kernel, tile=tile, tiles=tiles, lists=steps, period=period),
        grid_spec=pltpu.PrefetchScalarGridSpec(
            num_scalar_prefetch=2,
            grid=(steps + rows // (ROWS_OUT * out_rows),),
            in_specs=[
                pl.BlockSpec((together, 2, FIELDS, count // 2), lambda s, *_: (jnp.minimum(s, steps - 1), 0, 0, 0)),
                whole(low_table.shape),
                whole(high_table.shape),
                whole(one_table.shape),
                whole(cos.shape),
                whole(sin.shape),
                whole(two_table.shape),
            ],
            out_specs=pl.BlockSpec(
                (2, out_rows, blocks * ROWS_OUT, LANES), lambda s, *_: (0, jnp.maximum(s - steps, 0), 0, 0)
            ),
            scratch_shapes=[pltpu.VMEM(((blocks + WINDOW_BLOCKS) * (2 * rows + PAD), LANES), jnp.float32)]
            + [pltpu.VMEM((2 * rows, tile), jnp.bfloat16)] * (2 * tiles),
        ),
        out_shape=jax.ShapeDtypeStruct((2, rows // ROWS_OUT, blocks * ROWS_OUT, LANES), jnp.float32),
        compiler_params=pltpu.CompilerParams(vmem_limit_bytes=56 * MEBI),
    )(first, windows, gathered, low_table, high_table, one_table, cos, sin, two_table)
    picture = picture.reshape(2, rows // ROWS_OUT, blocks, ROWS_OUT, LANES)
    return jnp.transpose(picture, (0, 1, 3, 2, 4)).reshape(2, rows, GRID)


def solution(mesh):
    return jax.shard_map(
        on_device,
        mesh=mesh,
        in_specs=(
            P(None, ("au", "vert")),
            P(None, ("au", "vert")),
            P(None, ("au", "vert")),
            P(("au", "vert"), None),
            P(("au", "vert")),
            P(("au", "vert")),
        ),
        out_specs=P(None, ("au", "vert"), None),
        check_vma=False,
    )
```

```python
import functools
import math

import jax
import jax.numpy as jnp
import numpy as np
from jax import lax
from jax.experimental import pallas as pl
from jax.experimental.pallas import tpu as pltpu
from jax.sharding import PartitionSpec as P

GRID = 8192
TAPS = 16
LANES = 128
LOW = 128
FIELDS = 40
WINDOW_BLOCKS = 2
ROWS_OUT = 8
OUT_GROUPS = 2
PAD = 8
MEBI = 1024 * 1024


def phase_table(left, right, modulus):
    product = left[:, None] * right[None, :] % modulus
    angle = product.astype(jnp.float32) * (2.0 * math.pi / modulus)
    return jnp.cos(angle), jnp.sin(angle)


def rotated(taps, shift):
    tap = jnp.arange(TAPS, dtype=jnp.int32)[:, None]
    turned = jnp.zeros_like(taps)
    for t in range(TAPS):
        turned = turned + jnp.where((shift[None, :] + t) % TAPS == tap, taps[t : t + 1], 0)
    return turned


def spread_tile(fields, low_ref, high_ref, period):
    tile = fields.shape[1]
    taps_u = fields[TAPS : 2 * TAPS]
    extra = fields[2 * TAPS : 2 * TAPS + 8].astype(jnp.float32)
    row_high = extra[3:4].astype(jnp.bfloat16)
    row_mid = extra[4:5]
    row_low = extra[5:6]
    vis_re = extra[6:7].astype(jnp.bfloat16)
    vis_im = extra[7:8].astype(jnp.bfloat16)
    zero = jnp.zeros((), jnp.bfloat16)
    tap = lax.broadcasted_iota(jnp.int32, (TAPS, tile), 0).astype(jnp.float32)
    spot_u = (row_mid + jnp.where(tap < row_low, 1.0, 0.0)).astype(jnp.bfloat16)
    band_u = jnp.concatenate(
        [jnp.where(spot_u == jnp.bfloat16(q), taps_u, zero) for q in range(LOW // TAPS + 1)], axis=0
    )
    high_count = GRID // LOW
    number = lax.broadcasted_iota(jnp.int32, (high_count, tile), 0).astype(jnp.float32).astype(jnp.bfloat16)
    here = number == jnp.broadcast_to(row_high, (high_count, tile))
    picked = jnp.concatenate(
        [
            jnp.where(here, jnp.broadcast_to(vis_re, (high_count, tile)), zero),
            jnp.where(here, jnp.broadcast_to(vis_im, (high_count, tile)), zero),
        ],
        axis=0,
    )
    high = jnp.dot(high_ref[...], picked, preferred_element_type=jnp.float32)
    high_re, high_im = high[:period], high[period:]
    low = jnp.dot(low_ref[...], band_u, preferred_element_type=jnp.float32)
    parts = []
    for begin in range(0, low.shape[0], 2 * period):
        low_re = low[begin : begin + period]
        low_im = low[begin + period : begin + 2 * period]
        parts.append((low_re * high_re - low_im * high_im).astype(jnp.bfloat16))
        parts.append((low_re * high_im + low_im * high_re).astype(jnp.bfloat16))
    return jnp.concatenate(parts, axis=0)


def add_window(spread, fields, block, acc_ref):
    tile = fields.shape[1]
    taps_v = fields[0:TAPS]
    extra = fields[2 * TAPS : 2 * TAPS + 8].astype(jnp.float32)
    tap = lax.broadcasted_iota(jnp.int32, (TAPS, tile), 0).astype(jnp.float32)
    groups = LANES // TAPS
    count = WINDOW_BLOCKS * groups
    zero = jnp.zeros((), jnp.bfloat16)
    spot = (extra[0:1] - block.astype(jnp.float32)) * groups + extra[1:2] + jnp.where(tap < extra[2:3], 1.0, 0.0)
    near = jnp.clip(spot, -1.0, float(count)).astype(jnp.bfloat16)
    band_v = jnp.concatenate([jnp.where(near == jnp.bfloat16(q), taps_v, zero) for q in range(count)], axis=0)
    out = lax.dot_general(spread, band_v, (((1,), (1,)), ((), ())), preferred_element_type=jnp.float32)
    pitch = spread.shape[0] + PAD
    for j in range(WINDOW_BLOCKS):
        rows = pl.ds(pl.multiple_of((block + j) * pitch, PAD), spread.shape[0])
        acc_ref[rows, :] += out[:, j * LANES : (j + 1) * LANES]


def image_kernel(
    first_ref, extra_ref, pay_ref, low_ref, high_ref, one_ref, cos_ref, sin_ref, two_ref, out_ref, acc_ref, *spreads,
    tile, tiles, lists, period,
):
    step = pl.program_id(0)
    blocks = GRID // LANES
    pitch = low_ref.shape[0] + PAD

    @pl.when(step == 0)
    def _():
        def clear(n, carry):
            rows = pl.ds(pl.multiple_of(n * pitch, PAD), pitch)
            acc_ref[rows, :] = jnp.zeros((pitch, LANES), jnp.float32)
            return carry

        lax.fori_loop(0, acc_ref.shape[0] // pitch, clear, 0)

    @pl.when(step < lists)
    def _():
        def one_list(part, carry):
            place = (step * pay_ref.shape[0] + part) * 2 * tiles
            fields = lambda n: pay_ref[part, n // tiles, :, n % tiles * tile : (n % tiles + 1) * tile]
            for n in range(2 * tiles):
                spread = spread_tile(fields(n), low_ref, high_ref, period)
                spreads[n][...] = spread
                add_window(spread, fields(n), first_ref[place + n], acc_ref)
            for n in range(2 * tiles):
                def more(window, carry, n=n):
                    block = jnp.minimum(first_ref[place + n] + window * WINDOW_BLOCKS, blocks)
                    add_window(spreads[n][...], fields(n), block, acc_ref)
                    return carry

                lax.fori_loop(1, extra_ref[place + n], more, 0)
            return carry

        lax.fori_loop(0, pay_ref.shape[0], one_list, 0)

    @pl.when(step >= lists)
    def _():
        def some_rows(turn, carry):
            for group in range(OUT_GROUPS):
                here = turn * OUT_GROUPS + group
                first_row = ((step - lists) * out_ref.shape[1] + here) * ROWS_OUT
                at = first_row // period * (2 * period) + first_row % period
                image_rows(at, period, acc_ref, one_ref, cos_ref, sin_ref, two_ref, out_ref, here, pitch)
            return carry

        lax.fori_loop(0, out_ref.shape[1] // OUT_GROUPS, some_rows, 0)


def image_rows(at, period, acc_ref, one_ref, cos_ref, sin_ref, two_ref, out_ref, group, pitch):
    blocks = GRID // LANES
    row = lambda part, m: acc_ref[pl.ds(at + part * period + m, blocks, stride=pitch), :].astype(jnp.bfloat16)
    stack = jnp.concatenate(
        [jnp.concatenate([row(part, m) for m in range(ROWS_OUT)], axis=1) for part in range(2)], axis=0
    )
    mid = jnp.dot(one_ref[...], stack, preferred_element_type=jnp.float32)
    cos, sin = cos_ref[...], sin_ref[...]
    rows = []
    for m in range(ROWS_OUT):
        re = mid[:blocks, m * LANES : (m + 1) * LANES]
        im = mid[blocks:, m * LANES : (m + 1) * LANES]
        rows.append(
            jnp.concatenate(
                [(re * cos - im * sin).astype(jnp.bfloat16), (re * sin + im * cos).astype(jnp.bfloat16)], axis=1
            )
        )
    turned = jnp.concatenate(rows, axis=0)
    out = lax.dot_general(two_ref[...], turned, (((1,), (1,)), ((), ())), preferred_element_type=jnp.float32)
    half = LANES // 2
    left = lax.broadcasted_iota(jnp.int32, (half, LANES), 1) < half
    for part in range(2):
        for pair in range(ROWS_OUT // 2):
            lanes = slice(pair * LANES, (pair + 1) * LANES)
            even = out[2 * part * half : (2 * part + 1) * half, lanes]
            odd = out[(2 * part + 1) * half : (2 * part + 2) * half, lanes]
            put = lambda m: pl.ds(m, blocks, stride=ROWS_OUT)
            out_ref[part, group, put(2 * pair), :] = jnp.where(left, even, pltpu.roll(odd, half, 1))
            out_ref[part, group, put(2 * pair + 1), :] = jnp.where(left, pltpu.roll(even, half, 1), odd)


MESH = pl.DeviceIdType.MESH


def exchange_kernel(src_ref, dst_ref, send_sem, recv_sem, *, sizes):
    spot, near, me = {}, {}, 0
    for axis, size in sizes.items():
        near[axis] = lax.rem(lax.axis_index(axis), size)
        spot[axis] = lax.axis_index(axis) - near[axis]
        me = me * size + near[axis]
    total = math.prod(sizes.values())
    width = src_ref.shape[1] // total

    def peer(hop):
        index, device = 0, {}
        for place, (axis, size) in enumerate(sizes.items()):
            step = hop // math.prod(list(sizes.values())[place + 1 :]) % size
            digit = lax.rem(near[axis] + step, size) if step else near[axis]
            index = index * size + digit
            device[axis] = spot[axis] + digit
        return index, device

    barrier = pltpu.get_barrier_semaphore()
    for hop in range(1, total):
        pl.semaphore_signal(barrier, inc=1, device_id=peer(hop)[1], device_id_type=MESH)
    pl.semaphore_wait(barrier, total - 1)
    piece = lambda ref, n: ref.at[:, pl.ds(pl.multiple_of(n * width, width), width)]
    copies = []
    for hop in range(1, total):
        index, device = peer(hop)
        copy = pltpu.make_async_remote_copy(
            src_ref=piece(src_ref, index),
            dst_ref=piece(dst_ref, me),
            send_sem=send_sem.at[hop],
            recv_sem=recv_sem.at[hop],
            device_id=device,
            device_id_type=MESH,
        )
        copy.start()
        copies.append(copy)
    own = pltpu.make_async_copy(piece(src_ref, me), piece(dst_ref, me), send_sem.at[0])
    own.start()
    own.wait()
    for copy in copies:
        copy.wait()


def exchanged(payload, axis, number):
    sizes = {axis: math.gcd(lax.axis_size(axis), payload.shape[1] // LANES)}
    total = math.prod(sizes.values())
    return pl.pallas_call(
        functools.partial(exchange_kernel, sizes=sizes),
        in_specs=[pl.BlockSpec(memory_space=pltpu.HBM)],
        out_specs=pl.BlockSpec(memory_space=pltpu.HBM),
        out_shape=jax.ShapeDtypeStruct(payload.shape, payload.dtype),
        scratch_shapes=[pltpu.SemaphoreType.DMA((total,)), pltpu.SemaphoreType.DMA((total,))],
        compiler_params=pltpu.CompilerParams(collective_id=number, has_side_effects=True),
    )(payload)


def flipped(place, mask):
    bit = 1
    while bit <= mask:
        if mask & bit:
            place = place + bit - 2 * bit * lax.rem(place // bit, 2)
        bit *= 2
    return place


def gather_kernel(src_ref, out_ref, own_sem, send_sem, recv_sem):
    n_au, n_vert = lax.axis_size("au"), lax.axis_size("vert")
    a, v = lax.axis_index("au"), lax.axis_index("vert")
    width = out_ref.shape[3]
    inner, cores = math.gcd(n_au, 2), math.gcd(n_vert, 2)
    sizes = {"x": inner, "y": n_au // inner, "z": n_vert // cores, "c": cores}
    place = {"x": lax.rem(a, inner), "y": a // inner, "z": v // cores, "c": lax.rem(v, cores)}

    def at(**moved):
        spot = dict(place)
        for name, hop in moved.items():
            spot[name] = flipped(place[name], hop)
        return spot["y"] * inner + spot["x"], spot["z"] * cores + spot["c"]

    steps = [(name, hop) for name in "xyzc" for hop in range(1, sizes[name])]
    barrier = pltpu.get_barrier_semaphore()
    for name, hop in steps:
        au, vert = at(**{name: hop})
        pl.semaphore_signal(barrier, inc=1, device_id={"au": au, "vert": vert}, device_id_type=MESH)
    pl.semaphore_wait(barrier, len(steps))

    sent = []

    def send(half, source, moved, name, hop):
        au, vert = at(**moved)
        origin = au * n_vert + vert
        to_au, to_vert = at(**{name: hop})
        path = dict(moved)
        path[name] = hop
        slot = tuple(path.get(n, 0) for n in "xyzc")
        copy = pltpu.make_async_remote_copy(
            src_ref=source,
            dst_ref=out_ref.at[origin, half],
            send_sem=send_sem.at[len(sent)],
            recv_sem=recv_sem.at[number(half, slot)],
            device_id={"au": to_au, "vert": to_vert},
            device_id_type=MESH,
        )
        copy.start()
        sent.append(copy)

    def number(half, slot):
        total = half
        for n, d in zip("xyzc", slot):
            total = total * sizes[n] + d
        return total

    def arrived(half, moved):
        au, vert = at(**moved)
        block = out_ref.at[au * n_vert + vert, half]
        slot = tuple(moved.get(n, 0) for n in "xyzc")
        pltpu.make_async_copy(block, block, recv_sem.at[number(half, slot)]).wait()
        return block

    order = [("z", "x", "y", "c"), ("z", "y", "x", "c")]

    def pass_on(half, source, moved, stage):
        for name in order[half][stage:]:
            for hop in range(1, sizes[name]):
                send(half, source, moved, name, hop)

    halves = [src_ref.at[:, pl.ds(h * width, width)] for h in range(2)]
    for half in range(2):
        pass_on(half, halves[half], {}, 0)
    origin = a * n_vert + v
    keep = [pltpu.make_async_copy(halves[h], out_ref.at[origin, h], own_sem.at[h]) for h in range(2)]
    for copy in keep:
        copy.start()

    def along_z(hop_z):
        for half in range(2):
            pass_on(half, arrived(half, {"z": hop_z}), {"z": hop_z}, 1)

    def along_second(hop_z):
        for half in range(2):
            second = order[half][1]
            for hop in range(1, sizes[second]):
                moved = {"z": hop_z, second: hop}
                pass_on(half, arrived(half, moved), moved, 2)

    for hop_z in range(sizes["z"] + 1):
        if 0 < hop_z < sizes["z"]:
            along_z(hop_z)
        if hop_z != 1:
            along_second(max(hop_z - 1, 0))
    for hop_z in range(sizes["z"]):
        for half in range(2):
            second, third = order[half][1:3]
            for hop in range(sizes[second]):
                for hop_third in range(1, sizes[third]):
                    moved = {"z": hop_z, second: hop, third: hop_third}
                    pass_on(half, arrived(half, moved), moved, 3)
    for half in range(2):
        for hop in range(1, sizes["c"]):
            for x in range(sizes["x"]):
                for y in range(sizes["y"]):
                    for z in range(sizes["z"]):
                        arrived(half, {"c": hop, "x": x, "y": y, "z": z})
    for copy in keep:
        copy.wait()
    for copy in sent:
        copy.wait_send()


def gathered_everywhere(payload, devices, number):
    fields, count = payload.shape
    return pl.pallas_call(
        gather_kernel,
        in_specs=[pl.BlockSpec(memory_space=pltpu.VMEM)],
        out_specs=pl.BlockSpec(memory_space=pltpu.HBM),
        out_shape=jax.ShapeDtypeStruct((devices, 2, fields, count // 2), payload.dtype),
        scratch_shapes=[
            pltpu.SemaphoreType.DMA((2,)),
            pltpu.SemaphoreType.DMA((2 * devices,)),
            pltpu.SemaphoreType.DMA((2 * devices,)),
        ],
        compiler_params=pltpu.CompilerParams(collective_id=number, has_side_effects=True),
    )(payload)


def fixed_table(left, right, modulus):
    angle = np.outer(left, right) % modulus * (2.0 * math.pi / modulus)
    return np.cos(angle), np.sin(angle)


def stacked(cos, sin):
    return jnp.asarray(np.block([[cos, -sin], [sin, cos]]), dtype=jnp.bfloat16)


def columns_of(payload):
    ends = payload[..., 2 * TAPS : 2 * TAPS + 3, :].astype(jnp.int32)
    return ends[..., 0, :] * LANES + ends[..., 1, :] * TAPS + ends[..., 2, :]


def ordered(payload):
    count = payload.shape[1]
    key = columns_of(payload) * count + jnp.arange(count, dtype=jnp.int32)
    rank = jnp.sum((key[:, None] < key[None, :]).astype(jnp.int32), axis=0)
    order = (rank[:, None] == jnp.arange(count, dtype=jnp.int32)[None, :]).astype(jnp.bfloat16)
    return jnp.dot(payload, order, preferred_element_type=jnp.float32).astype(jnp.bfloat16)


def on_device(visibility, taps_u, taps_v, facet, u_offset, v_offset):
    n_au = lax.axis_size("au")
    n_vert = lax.axis_size("vert")
    devices = n_au * n_vert
    count = visibility.shape[1]
    rows = GRID // devices
    own = lax.axis_index("au") * n_vert + lax.axis_index("vert")
    target = facet[:, 0]
    row = target // n_vert * (GRID // n_au) + u_offset
    col = target % n_vert * (GRID // n_vert) + v_offset
    scalars = jnp.stack(
        [col // LANES, col % LANES // TAPS, col % TAPS, row // LOW, row % LOW // TAPS, row % TAPS]
    ).astype(jnp.bfloat16)
    payload = jnp.concatenate(
        [rotated(taps_v, col % TAPS), rotated(taps_u, row % TAPS), scalars, visibility], axis=0
    )
    payload = ordered(payload)
    payload = exchanged(payload, "vert", 0)
    payload = ordered(payload)
    payload = exchanged(payload, "au", 1)
    payload = ordered(payload)
    gathered = gathered_everywhere(payload, devices, 2)
    tile = math.gcd(count // 2, 256)
    tiles = count // 2 // tile
    blocks = GRID // LANES
    columns = columns_of(gathered).reshape(-1, tile)
    first = jnp.min(columns, axis=1) // LANES
    windows = ((jnp.max(columns, axis=1) + TAPS - 1) // LANES - first) // WINDOW_BLOCKS + 1

    k = own * rows + jnp.arange(rows, dtype=jnp.int32)
    high_count = GRID // LOW
    period = min(rows, high_count)
    low_cos, low_sin = phase_table(k, jnp.arange(LOW + TAPS, dtype=jnp.int32), GRID)
    low_table = jnp.concatenate(
        [low_cos.reshape(rows // period, 1, period, -1), low_sin.reshape(rows // period, 1, period, -1)], axis=1
    ).reshape(2 * rows, -1).astype(jnp.bfloat16)
    turns = phase_table(k[:period], jnp.arange(high_count, dtype=jnp.int32), high_count)
    high_table = jnp.block([[turns[0], -turns[1]], [turns[1], turns[0]]]).astype(jnp.bfloat16)

    a, b = np.arange(blocks), np.arange(LANES)
    one_table = stacked(*fixed_table(a, a, blocks))
    cos, sin = fixed_table(a, b, GRID)
    scale = 1.0 / math.sqrt(count * devices)
    mu = np.concatenate([np.arange(0, LANES, 2), np.arange(1, LANES, 2)])
    two_table = stacked(*fixed_table(mu, b, LANES))
    cos, sin = jnp.asarray(cos * scale, dtype=jnp.float32), jnp.asarray(sin * scale, dtype=jnp.float32)
    together = math.gcd(devices, 4)
    steps = devices // together
    out_rows = OUT_GROUPS * math.gcd(rows // (ROWS_OUT * OUT_GROUPS), 2)
    whole = lambda shape: pl.BlockSpec(shape, lambda n, *_: (0,) * len(shape))
    picture = pl.pallas_call(
        functools.partial(image_kernel, tile=tile, tiles=tiles, lists=steps, period=period),
        grid_spec=pltpu.PrefetchScalarGridSpec(
            num_scalar_prefetch=2,
            grid=(steps + rows // (ROWS_OUT * out_rows),),
            in_specs=[
                pl.BlockSpec((together, 2, FIELDS, count // 2), lambda s, *_: (jnp.minimum(s, steps - 1), 0, 0, 0)),
                whole(low_table.shape),
                whole(high_table.shape),
                whole(one_table.shape),
                whole(cos.shape),
                whole(sin.shape),
                whole(two_table.shape),
            ],
            out_specs=pl.BlockSpec(
                (2, out_rows, blocks * ROWS_OUT, LANES), lambda s, *_: (0, jnp.maximum(s - steps, 0), 0, 0)
            ),
            scratch_shapes=[pltpu.VMEM(((blocks + WINDOW_BLOCKS) * (2 * rows + PAD), LANES), jnp.float32)]
            + [pltpu.VMEM((2 * rows, tile), jnp.bfloat16)] * (2 * tiles),
        ),
        out_shape=jax.ShapeDtypeStruct((2, rows // ROWS_OUT, blocks * ROWS_OUT, LANES), jnp.float32),
        compiler_params=pltpu.CompilerParams(vmem_limit_bytes=56 * MEBI),
    )(first, windows, gathered, low_table, high_table, one_table, cos, sin, two_table)
    picture = picture.reshape(2, rows // ROWS_OUT, blocks, ROWS_OUT, LANES)
    return jnp.transpose(picture, (0, 1, 3, 2, 4)).reshape(2, rows, GRID)


def solution(mesh):
    return jax.shard_map(
        on_device,
        mesh=mesh,
        in_specs=(
            P(None, ("au", "vert")),
            P(None, ("au", "vert")),
            P(None, ("au", "vert")),
            P(("au", "vert"), None),
            P(("au", "vert")),
            P(("au", "vert")),
        ),
        out_specs=P(None, ("au", "vert"), None),
        check_vma=False,
    )
```
